32 devices in a mesh: groups: 2 (over y), wide: 4 (over z), narrow: 4 (over x, core).
Axes of the slice: x: 2, y: 2, z: 4, core: 2. Of those that a mesh axis runs over, the one named last changes fastest.
Arguments:
- cont_queries: bfloat16 [32, 128, 64, 128], P(('groups', 'wide'), None, 'narrow'), parts along dimension 0, may hold values from -5 to 5
- cont_keys: bfloat16 [32, 128, 8, 128], P(('groups', 'wide'), None, 'narrow'), parts along dimension 0, may hold values from -5 to 5
- cont_values: bfloat16 [32, 128, 8, 128], P(('groups', 'wide'), None, 'narrow'), parts along dimension 0, may hold values from -5 to 5
- prefix_kv: bfloat16 [8, 2, 128, 8, 128], P(('groups', 'wide'), None, None, 'narrow'), parts along dimension 0, may hold values from -5 to 5
- probe: bfloat16 [64, 128], P('narrow'), may hold values from -0.5 to 0.5
- question_row: int32 [8], P('groups'), parts along dimension 0, may hold values from 0 to 3, each once
- cont_slot: int32 [32], P(('groups', 'wide')), parts along dimension 0, may hold values from 0 to 15, each once
- cont_length: int32 [32], P(('groups', 'wide')), parts along dimension 0, may hold values from 1 to 128
- gold: int32 [8], P('groups'), parts along dimension 0, may hold values from 0 to 3
Outputs:
- token_score: float32 [32, 128], P(('groups', 'wide')), parts along dimension 0
- owned_logprob: float32 [8, 4], P(('groups', 'wide')), parts along dimension 0
- owned_loss: float32 [8], P(('groups', 'wide')), parts along dimension 0
The draws below stay inside these ranges and needn't reach their ends.
There are 2 independent parts, one for each index of `groups`. The reference program is written for one: setup_inputs(seed, part) draws one part's arguments, and reference() takes and returns one part's arrays. A program takes and returns all parts, laid end to end along the dimension named above; an argument that names none is the same for every part. Nothing has to cross between parts.
All inputs are finite; a program needn't handle non-finite values.
Results may differ from the reference program's by a relative error of at most 0.0065.
Values may be sent and summed in bfloat16 or wider, within the bound.
A program may use at most 64 MiB of HBM per device.

```python
import jax
import jax.numpy as jnp
from jax import lax

HEADS = 64
KV_HEADS = 8
HEAD_DIM = 128
ANSWERS = 4
CLEN = 128
PREF = 128
QUESTIONS = 4
CONTS = 16


def draw_cont_queries(key, part):
    drawn = jax.random.normal(jax.random.fold_in(key, 1), (CONTS, CLEN, HEADS, HEAD_DIM), jnp.float32)
    drawn = jnp.clip(drawn, -5.0, 5.0)
    return drawn.astype(jnp.bfloat16)


def draw_prefix_kv(key, part):
    drawn = jax.random.normal(jax.random.fold_in(key, 2), (QUESTIONS, 2, PREF, KV_HEADS, HEAD_DIM), jnp.float32)
    drawn = jnp.clip(drawn, -5.0, 5.0)
    return drawn.astype(jnp.bfloat16)


def plant(values, rng, least, top_value):
    dims = values.shape
    index_at = [jax.random.randint(jax.random.fold_in(rng, axis), (), 0, dims[axis]) for axis in range(len(dims))]
    values = values.at[tuple(index_at)].set(least)
    longest = dims.index(max(dims))
    index_at[longest] = (index_at[longest] + 1) % dims[longest]
    return values.at[tuple(index_at)].set(top_value)


def steps_of(own_key, dims, cuts, low, top_value):
    gain = 1.0
    for dim, blocks in cuts:
        steps = jax.random.uniform(jax.random.fold_in(jax.random.fold_in(own_key, 6), dim), (blocks,), jnp.float32, low / len(cuts), top_value / len(cuts))
        gain = gain * jnp.repeat(jnp.exp(steps), dims[dim] // blocks).reshape((-1,) + (1,) * (len(dims) - 1 - dim))
    return gain


def noise(own_key, shape, spread, limit, split=(), held_as=jnp.bfloat16):
    result = jax.random.normal(own_key, shape, jnp.float32) * spread
    if len(split) > 0:
        result = steps_of(own_key, shape, split, -0.22, 0.18) * result
    return jnp.clip(result, min=-limit, max=limit).astype(held_as)


def setup_inputs(seed: int = 0, part: int = 0) -> dict:
    key_list = jax.random.split(jax.random.key(seed), 10)
    own_keys = jax.random.split(jax.random.fold_in(key_list[9], part), 10)
    return {
        "cont_queries": draw_cont_queries(jax.random.fold_in(jax.random.fold_in(key_list[9], part), 71), part),
        "cont_keys": noise(own_keys[1], (CONTS, CLEN, KV_HEADS, HEAD_DIM), 1.0, 5.0, ((0, 4), (2, 4))),
        "cont_values": noise(own_keys[2], (CONTS, CLEN, KV_HEADS, HEAD_DIM), 1.0, 5.0, ((0, 4), (2, 4))),
        "prefix_kv": draw_prefix_kv(jax.random.fold_in(jax.random.fold_in(key_list[9], part), 71), part),
        "probe": noise(key_list[4], (HEADS, HEAD_DIM), HEAD_DIM ** -0.5, 0.5, ((0, 4),)),
        "question_row": jax.random.permutation(own_keys[5], QUESTIONS).astype(jnp.int32),
        "cont_slot": jax.random.permutation(own_keys[6], CONTS).astype(jnp.int32),
        "cont_length": plant(jax.random.randint(own_keys[7], (CONTS,), 1, CLEN + 1), jax.random.fold_in(own_keys[7], 1), 1, CLEN).astype(jnp.int32),
        "gold": plant(jax.random.randint(own_keys[8], (QUESTIONS,), 0, ANSWERS), jax.random.fold_in(own_keys[8], 1), 0, ANSWERS - 1).astype(jnp.int32),
    }


def reference(cont_queries, cont_keys, cont_values, prefix_kv, probe, question_row, cont_slot, cont_length, gold):
    group_size = HEADS // KV_HEADS
    scale_factor = 1.0 / (HEAD_DIM ** 0.5)
    wanted = question_row[cont_slot // ANSWERS].astype(jnp.int32)
    causal = jnp.arange(CLEN)[:, None] >= jnp.arange(CLEN)[None, :]
    allowed = jnp.concatenate([jnp.ones((CLEN, PREF), dtype=bool), causal], axis=1)

    def score_one(packed):
        queries, keys_own, values_own, prefix_row = packed
        cached = lax.dynamic_index_in_dim(prefix_kv, prefix_row, 0, keepdims=False)
        keys_all = jnp.concatenate([cached[0], keys_own], axis=0)
        values_all = jnp.concatenate([cached[1], values_own], axis=0)
        keys_wide = jnp.repeat(keys_all, group_size, axis=1).astype(jnp.float32)
        values_wide = jnp.repeat(values_all, group_size, axis=1).astype(jnp.float32)
        scores = jnp.einsum("thd,jhd->htj", queries.astype(jnp.float32), keys_wide) * scale_factor
        scores = jnp.where(allowed[None, :, :], scores, -jnp.inf)
        row_max = jnp.max(scores, axis=-1, keepdims=True)
        expo = jnp.exp(scores - row_max)
        total = jnp.sum(expo, axis=-1)
        weights = expo.astype(jnp.bfloat16)
        summed = jnp.einsum("htj,jhd->thd", weights.astype(jnp.float32), values_wide)
        attended = (summed / jnp.transpose(total)[:, :, None]).astype(jnp.bfloat16)
        return jnp.einsum("thd,hd->t", attended.astype(jnp.float32), probe.astype(jnp.float32))

    token_score = lax.map(score_one, (cont_queries, cont_keys, cont_values, wanted))
    valid = jnp.arange(CLEN)[None, :] < cont_length[:, None]
    choice_score = jnp.sum(jnp.where(valid, token_score, jnp.zeros_like(token_score)), axis=1)
    question_score = jnp.zeros((QUESTIONS * ANSWERS,), jnp.float32).astype(choice_score.dtype)
    question_score = question_score.at[cont_slot].set(choice_score).reshape(QUESTIONS, ANSWERS)
    logprob = question_score - jax.nn.logsumexp(question_score, axis=1, keepdims=True)
    owned_logprob = jnp.zeros_like(logprob).at[question_row].set(logprob)
    picked = jnp.take_along_axis(logprob, gold[:, None].astype(jnp.int32), axis=1)[:, 0]
    owned_loss = jnp.zeros_like(picked).at[question_row].set(-picked)
    return token_score, owned_logprob, owned_loss
```

```python
import functools

import jax
import jax.numpy as jnp
from jax import lax
from jax.experimental import pallas as pl
from jax.experimental.pallas import tpu as pltpu
from jax.sharding import PartitionSpec as P

MESH = pl.DeviceIdType.MESH
ANSWERS = 4
LANES = 128
NEG = -1e30
LOG2E = 1.4426950408889634
F32 = jnp.float32
BF16 = jnp.bfloat16
NT = (((1,), (1,)), ((), ()))
TN = (((0,), (0,)), ((), ()))


def iota(shape, dim):
    return lax.broadcasted_iota(jnp.int32, shape, dim)


def kernel(
    sizes,
    qrow_ref, slot_ref, len_ref, gold_ref, q_hbm, k_hbm, v_hbm, pre_hbm, probe_ref,
    tok_ref, logp_ref, loss_ref,
    q_v, k_v, v_v, pv_v, kslot, vpslot, split, kown, vpt, kpre, vptp,
    m1, l1, n1, m2, l2, n2, tslot, cbuf, cslot,
    in_sem, ksend, krecv, vsend, vrecv, tsend, trecv, csend, crecv,
):
    wide, narrow, conts, clen, heads, kv, dim, quest, pref, questions = sizes
    group = heads // kv
    scale = LOG2E / dim**0.5
    me_w = lax.axis_index("wide")
    me_n = lax.axis_index("narrow")
    tcols = 2 * LANES // heads
    cols = tcols * heads
    blocks = clen // tcols
    own = pl.ds(me_w * quest, quest)

    cp_k = pltpu.make_async_copy(pre_hbm.at[:, 0], kslot.at[own], in_sem.at[0])
    cp_v = pltpu.make_async_copy(pre_hbm.at[:, 1], pv_v, in_sem.at[1])
    cp_ko = pltpu.make_async_copy(k_hbm, k_v, in_sem.at[2])
    cp_vo = pltpu.make_async_copy(v_hbm, v_v, in_sem.at[3])
    cp_q = pltpu.make_async_copy(q_hbm, q_v, in_sem.at[4])
    for cp in (cp_k, cp_v, cp_ko, cp_vo, cp_q):
        cp.start()

    barrier = pltpu.get_barrier_semaphore()
    total = wide * narrow
    me = me_w * narrow + me_n

    def peer(i):
        p = lax.rem(me + i, total)
        return {"wide": lax.div(p, narrow), "narrow": lax.rem(p, narrow)}

    def greet(i, _):
        pl.semaphore_signal(barrier, inc=1, device_id=peer(i), device_id_type=MESH)
        return 0

    lax.fori_loop(1, total, greet, 0)

    probe = probe_ref[...]
    lane = iota((1, LANES), 1)
    lane_kv = (lane % heads) // group
    rowsel = iota((LANES, heads), 0) % heads == iota((LANES, heads), 1)
    tile_mat = jnp.where(rowsel, 1.0, 0.0).astype(BF16)
    probe_t = lax.dot_general(
        tile_mat, probe, (((1,), (0,)), ((), ())), preferred_element_type=F32
    ).astype(BF16)
    expand = jnp.where(iota((heads, LANES), 1) % heads == iota((heads, LANES), 0), 1.0, 0.0)

    def unpack(x):
        split[...] = x.astype(F32)
        n = x.shape[0] // kv
        return [split[pl.ds(i, n, stride=kv), :] for i in range(kv)]

    cp_v.wait()
    head_kv = iota((heads, 1), 0) // group
    for r in range(quest):
        acc = jnp.zeros((heads, pref), F32)
        for i, part in enumerate(unpack(pv_v[r])):
            d = lax.dot_general(probe, part.astype(BF16), NT, preferred_element_type=F32)
            acc = jnp.where(head_kv == i, d, acc)
        vpslot[me_w * quest + r] = acc
    cp_k.wait()
    pl.semaphore_wait(barrier, total - 1)

    def wpeer(i):
        return lax.rem(me_w + i, wide)

    def kcopy(i):
        return pltpu.make_async_remote_copy(
            src_ref=kslot.at[own], dst_ref=kslot.at[own],
            send_sem=ksend.at[i - 1], recv_sem=krecv.at[i - 1],
            device_id={"wide": wpeer(i)}, device_id_type=MESH,
        )

    def vcopy(i):
        return pltpu.make_async_remote_copy(
            src_ref=vpslot.at[own], dst_ref=vpslot.at[own],
            send_sem=vsend.at[i - 1], recv_sem=vrecv.at[i - 1],
            device_id={"wide": wpeer(i)}, device_id_type=MESH,
        )

    def each_peer(count, fn):
        def step(i, _):
            fn(i)
            return 0
        lax.fori_loop(1, count, step, 0)

    each_peer(wide, lambda i: kcopy(i).start())
    each_peer(wide, lambda i: vcopy(i).start())

    def start_mask(c, b):
        rows = q_v[c, pl.ds(b * cols, cols), :]
        rk = (iota((cols, 1), 0) % heads) // group
        return jnp.concatenate(
            [rows * jnp.where(rk == i, 1.0, 0.0).astype(BF16) for i in range(kv)], axis=1
        )

    def softmax_part(s, vp):
        m = jnp.max(s, axis=0, keepdims=True)
        e = jnp.exp2((s - m) * scale)
        l = jnp.sum(e, axis=0, keepdims=True)
        n = jnp.sum(e * jnp.concatenate([vp] * (cols // LANES), axis=1), axis=0, keepdims=True)
        return m, l, n

    cp_ko.wait()
    cp_vo.wait()
    cp_q.wait()

    def own_part(c, _):
        parts = unpack(k_v[c])
        for i in range(kv):
            kown[:, i * dim:(i + 1) * dim] = parts[i].astype(BF16)
        d = lax.dot_general(v_v[c], probe_t, NT, preferred_element_type=F32)
        split[...] = d
        acc = split[pl.ds(0, clen, stride=kv), :]
        for i in range(1, kv):
            acc = jnp.where(lane_kv == i, split[pl.ds(i, clen, stride=kv), :], acc)
        vpt[...] = acc
        for b in range(blocks):
            n_rows = (b + 1) * tcols
            q2 = start_mask(c, b)
            s = lax.dot_general(kown[:n_rows, :], q2, NT, preferred_element_type=F32)
            ok = iota((tcols, cols), 0) <= iota((tcols, cols), 1) // heads
            last = jnp.where(ok, s[n_rows - tcols:], NEG)
            s = last if b == 0 else jnp.concatenate([s[:n_rows - tcols], last], axis=0)
            m, l, n = softmax_part(s, vpt[:n_rows, :])
            m1[c, b:b + 1, :] = m
            l1[c, b:b + 1, :] = l
            n1[c, b:b + 1, :] = n
        return 0

    lax.fori_loop(0, conts, own_part, 0)

    each_peer(wide, lambda i: kcopy(i).wait())
    each_peer(wide, lambda i: vcopy(i).wait())

    def prefix_part(c, _):
        w = qrow_ref[slot_ref[c] // ANSWERS]
        parts = unpack(kslot[w])
        for i in range(kv):
            kpre[:, i * dim:(i + 1) * dim] = parts[i].astype(BF16)
        vptp[...] = lax.dot_general(
            vpslot[w], expand, TN, preferred_element_type=F32, precision=lax.Precision.HIGHEST
        )
        for b in range(blocks):
            q2 = start_mask(c, b)
            s = lax.dot_general(kpre[...], q2, NT, preferred_element_type=F32)
            m, l, n = softmax_part(s, vptp[...])
            m2[c, b:b + 1, :] = m
            l2[c, b:b + 1, :] = l
            n2[c, b:b + 1, :] = n
        return 0

    lax.fori_loop(0, conts, prefix_part, 0)

    fold = jnp.where(iota((cols, clen), 0) // heads == iota((cols, clen), 1) % tcols, 1.0, 0.0)
    keep = iota((blocks, clen), 1) // tcols == iota((blocks, clen), 0)
    row_id = iota((conts, clen), 0)
    partial = jnp.zeros((conts, clen), F32)
    for c in range(conts):
        ma, mb = m1[c], m2[c]
        m = jnp.maximum(ma, mb)
        ea, eb = jnp.exp2((ma - m) * scale), jnp.exp2((mb - m) * scale)
        ratio = (n1[c] * ea + n2[c] * eb) / (l1[c] * ea + l2[c] * eb)
        y = jnp.dot(ratio, fold, preferred_element_type=F32, precision=lax.Precision.HIGHEST)
        y = jnp.sum(jnp.where(keep, y, 0.0), axis=0, keepdims=True)
        partial = jnp.where(row_id == c, y, partial)
    tslot[me_n] = partial

    choice_rows = wide * quest
    crow = iota((wide, quest, LANES), 0) * quest + iota((wide, quest, LANES), 1)
    clane = iota((wide, quest, LANES), 2)
    term = jnp.zeros((wide, quest, LANES), F32)
    tpos = iota((1, clen), 1)
    for c in range(conts):
        slot = slot_ref[c]
        w = qrow_ref[slot // ANSWERS]
        a = slot % ANSWERS
        val = jnp.sum(jnp.where(tpos < len_ref[c], partial[c:c + 1, :], 0.0), axis=1, keepdims=True)
        term = term + jnp.where((crow == w) & (clane == a), val.reshape(1, 1, 1), 0.0)
    cbuf[...] = term

    def tcopy(i):
        return pltpu.make_async_remote_copy(
            src_ref=tslot.at[me_n], dst_ref=tslot.at[me_n],
            send_sem=tsend.at[i - 1], recv_sem=trecv.at[i - 1],
            device_id={"narrow": lax.rem(me_n + i, narrow)}, device_id_type=MESH,
        )

    def ccopy(i):
        to = peer(i)
        return pltpu.make_async_remote_copy(
            src_ref=cbuf.at[to["wide"]], dst_ref=cslot.at[me],
            send_sem=csend.at[i - 1], recv_sem=crecv.at[i - 1],
            device_id=to, device_id_type=MESH,
        )

    each_peer(total, lambda i: ccopy(i).start())
    each_peer(narrow, lambda i: tcopy(i).start())
    cslot[me] = cbuf[me_w]

    each_peer(narrow, lambda i: tcopy(i).wait())
    tok = tslot[0]
    for i in range(1, narrow):
        tok = tok + tslot[i]
    tok_ref[...] = tok

    each_peer(total, lambda i: ccopy(i).wait())
    scores = jnp.sum(cslot[...], axis=0)
    live = iota((quest, LANES), 1) < ANSWERS
    masked = jnp.where(live, scores, NEG)
    top = jnp.max(masked, axis=1, keepdims=True)
    norm = jnp.log(jnp.sum(jnp.where(live, jnp.exp(masked - top), 0.0), axis=1, keepdims=True))
    logp = scores - top - norm
    logp_ref[...] = logp[:, :ANSWERS]
    mine = me_w * quest + iota((quest, 1), 0)
    gold = jnp.zeros((quest, 1), jnp.int32)
    for g in range(questions):
        gold = jnp.where(mine == qrow_ref[g], gold_ref[g], gold)
    pick = iota((quest, LANES), 1) == gold
    loss_ref[...] = -jnp.sum(jnp.where(pick, logp, 0.0), axis=1, keepdims=True)


def solution(mesh):
    wide, narrow = mesh.shape["wide"], mesh.shape["narrow"]
    total = wide * narrow

    def per_device(q, k, v, prefix, probe, qrow, slot, length, gold):
        conts, clen, heads, dim = q.shape
        kv = k.shape[2]
        quest, _, pref = prefix.shape[:3]
        questions = qrow.shape[0]
        cols = 2 * LANES // heads * heads
        blocks = clen * heads // cols
        sizes = (wide, narrow, conts, clen, heads, kv, dim, quest, pref, questions)
        smem = pl.BlockSpec(memory_space=pltpu.SMEM)
        vmem = pl.BlockSpec(memory_space=pltpu.VMEM)
        anyw = pl.BlockSpec(memory_space=pl.ANY)
        stat = pltpu.VMEM((conts, blocks, cols), F32)
        dma = pltpu.SemaphoreType.DMA
        tok, logp, loss = pl.pallas_call(
            functools.partial(kernel, sizes),
            out_shape=(
                jax.ShapeDtypeStruct((conts, clen), F32),
                jax.ShapeDtypeStruct((quest, ANSWERS), F32),
                jax.ShapeDtypeStruct((quest, 1), F32),
            ),
            in_specs=[smem] * 4 + [anyw] * 4 + [vmem],
            out_specs=(vmem, vmem, vmem),
            scratch_shapes=[
                pltpu.VMEM((conts, clen * heads, dim), BF16),
                pltpu.VMEM((conts, clen * kv, dim), BF16),
                pltpu.VMEM((conts, clen * kv, dim), BF16),
                pltpu.VMEM((quest, pref * kv, dim), BF16),
                pltpu.VMEM((wide * quest, pref * kv, dim), BF16),
                pltpu.VMEM((wide * quest, heads, pref), F32),
                pltpu.VMEM((clen * kv, dim), F32),
                pltpu.VMEM((clen, kv * dim), BF16),
                pltpu.VMEM((clen, LANES), F32),
                pltpu.VMEM((pref, kv * dim), BF16),
                pltpu.VMEM((pref, LANES), F32),
                stat, stat, stat, stat, stat, stat,
                pltpu.VMEM((narrow, conts, clen), F32),
                pltpu.VMEM((wide, quest, LANES), F32),
                pltpu.VMEM((total, quest, LANES), F32),
                dma((5,)),
                dma((wide - 1,)), dma((wide - 1,)), dma((wide - 1,)), dma((wide - 1,)),
                dma((narrow - 1,)), dma((narrow - 1,)), dma((total - 1,)), dma((total - 1,)),
            ],
            compiler_params=pltpu.CompilerParams(collective_id=0, has_side_effects=True),
        )(
            qrow, slot, length, gold,
            q.reshape(conts, clen * heads, dim),
            k.reshape(conts, clen * kv, dim),
            v.reshape(conts, clen * kv, dim),
            prefix.reshape(quest, 2, pref * kv, dim),
            probe,
        )
        return tok, logp, loss.reshape(quest)

    return jax.shard_map(
        per_device,
        mesh=mesh,
        in_specs=(
            P(("groups", "wide"), None, "narrow", None),
            P(("groups", "wide"), None, "narrow", None),
            P(("groups", "wide"), None, "narrow", None),
            P(("groups", "wide"), None, None, "narrow", None),
            P("narrow", None),
            P("groups"),
            P(("groups", "wide")),
            P(("groups", "wide")),
            P("groups"),
        ),
        out_specs=(P(("groups", "wide"), None), P(("groups", "wide"), None), P(("groups", "wide"))),
        check_vma=False,
    )
```

```python
import functools

import jax
import jax.numpy as jnp
from jax import lax
from jax.experimental import pallas as pl
from jax.experimental.pallas import tpu as pltpu
from jax.sharding import PartitionSpec as P

MESH = pl.DeviceIdType.MESH
ANSWERS = 4
LANES = 128
NEG = -1e30
LOG2E = 1.4426950408889634
F32 = jnp.float32
BF16 = jnp.bfloat16
NT = (((1,), (1,)), ((), ()))
TN = (((0,), (0,)), ((), ()))


def iota(shape, dim):
    return lax.broadcasted_iota(jnp.int32, shape, dim)


def kernel(
    sizes,
    qrow_ref, slot_ref, len_ref, gold_ref, q_hbm, k_hbm, v_hbm, pre_hbm, probe_ref,
    out_ref,
    q_v, k_v, v_v, pv_v, kslot, vpslot, split, kown, vpt, kpre, vptp,
    m1, l1, n1, m2, l2, n2, tslot, cbuf, cslot,
    in_sem, ksend, krecv, vsend, vrecv, tsend, trecv, csend, crecv,
):
    wide, narrow, conts, clen, heads, kv, dim, quest, pref, questions = sizes
    group = heads // kv
    scale = LOG2E / dim**0.5
    me_w = lax.axis_index("wide")
    me_n = lax.axis_index("narrow")
    tcols = 2 * LANES // heads
    cols = tcols * heads
    blocks = clen // tcols
    own = pl.ds(me_w * quest, quest)

    cp_k = pltpu.make_async_copy(pre_hbm.at[:, 0], kslot.at[own], in_sem.at[0])
    cp_v = pltpu.make_async_copy(pre_hbm.at[:, 1], pv_v, in_sem.at[1])
    cp_ko = pltpu.make_async_copy(k_hbm, k_v, in_sem.at[2])
    cp_vo = pltpu.make_async_copy(v_hbm, v_v, in_sem.at[3])
    cp_q = pltpu.make_async_copy(q_hbm, q_v, in_sem.at[4])
    for cp in (cp_k, cp_v, cp_ko, cp_vo, cp_q):
        cp.start()

    total = wide * narrow
    me = me_w * narrow + me_n
    right, left = lax.rem(me_w + 1, wide), lax.rem(me_w + wide - 1, wide)

    def peer(i):
        p = lax.rem(me + i, total)
        return {"wide": lax.div(p, narrow), "narrow": lax.rem(p, narrow)}

    barrier = pltpu.get_barrier_semaphore()
    near = [{"wide": right}, {"wide": left}]
    near += [{"narrow": lax.rem(me_n + i, narrow)} for i in range(1, narrow)]
    for to in near:
        pl.semaphore_signal(barrier, inc=1, device_id=to, device_id_type=MESH)

    probe = probe_ref[...]
    lane = iota((1, LANES), 1)
    lane_kv = (lane % heads) // group
    rowsel = iota((LANES, heads), 0) % heads == iota((LANES, heads), 1)
    tile_mat = jnp.where(rowsel, 1.0, 0.0).astype(BF16)
    probe_t = lax.dot_general(
        tile_mat, probe, (((1,), (0,)), ((), ())), preferred_element_type=F32
    ).astype(BF16)
    expand = jnp.where(iota((heads, LANES), 1) % heads == iota((heads, LANES), 0), 1.0, 0.0)

    def unpack(x):
        split[...] = x.astype(F32)
        n = x.shape[0] // kv
        return [split[pl.ds(i, n, stride=kv), :] for i in range(kv)]

    cp_v.wait()
    head_kv = iota((heads, 1), 0) // group
    for r in range(quest):
        acc = jnp.zeros((heads, pref), F32)
        for i, part in enumerate(unpack(pv_v[r])):
            d = lax.dot_general(probe, part.astype(BF16), NT, preferred_element_type=F32)
            acc = jnp.where(head_kv == i, d, acc)
        vpslot[me_w * quest + r] = acc
    cp_k.wait()
    pl.semaphore_wait(barrier, len(near))

    steps = wide // 2

    def ring_copy(buf, sends, recvs, step, way, half):
        size = buf.shape[1] // 2
        row = lax.rem(me_w + (wide - step + 1 if way == 0 else step - 1), wide)
        part = buf.at[pl.ds(row * quest, quest), pl.ds(half * size, size)]
        n = ((step - 1) * 2 + way) * 2 + half
        return pltpu.make_async_remote_copy(
            src_ref=part, dst_ref=part, send_sem=sends.at[n], recv_sem=recvs.at[n],
            device_id={"wide": right if way == 0 else left}, device_id_type=MESH,
        )

    def ring_step(step):
        out = []
        for turn in range(2 if step < steps else 1):
            for way in range(2):
                half = way if turn == 0 else 1 - way
                for args in ((vpslot, vsend, vrecv), (kslot, ksend, krecv)):
                    out.append(ring_copy(*args, step, way, half))
        return out

    pending = ring_step(1)
    for cp in pending:
        cp.start()

    def each_peer(count, fn):
        def step(i, _):
            fn(i)
            return 0
        lax.fori_loop(1, count, step, 0)

    def start_mask(c, b):
        rows = q_v[c, pl.ds(b * cols, cols), :]
        rk = (iota((cols, 1), 0) % heads) // group
        return jnp.concatenate(
            [rows * jnp.where(rk == i, 1.0, 0.0).astype(BF16) for i in range(kv)], axis=1
        )

    def softmax_part(s, vp):
        m = jnp.max(s, axis=0, keepdims=True)
        e = jnp.exp2((s - m) * scale)
        l = jnp.sum(e, axis=0, keepdims=True)
        n = jnp.sum(e * jnp.concatenate([vp] * (cols // LANES), axis=1), axis=0, keepdims=True)
        return m, l, n

    cp_ko.wait()
    cp_vo.wait()
    cp_q.wait()

    def own_part(c, _):
        parts = unpack(k_v[c])
        for i in range(kv):
            kown[:, i * dim:(i + 1) * dim] = parts[i].astype(BF16)
        d = lax.dot_general(v_v[c], probe_t, NT, preferred_element_type=F32)
        split[...] = d
        acc = split[pl.ds(0, clen, stride=kv), :]
        for i in range(1, kv):
            acc = jnp.where(lane_kv == i, split[pl.ds(i, clen, stride=kv), :], acc)
        vpt[...] = acc
        for b in range(blocks):
            n_rows = (b + 1) * tcols
            q2 = start_mask(c, b)
            s = lax.dot_general(kown[:n_rows, :], q2, NT, preferred_element_type=F32)
            ok = iota((tcols, cols), 0) <= iota((tcols, cols), 1) // heads
            last = jnp.where(ok, s[n_rows - tcols:], NEG)
            s = last if b == 0 else jnp.concatenate([s[:n_rows - tcols], last], axis=0)
            m, l, n = softmax_part(s, vpt[:n_rows, :])
            m1[c, b:b + 1, :] = m
            l1[c, b:b + 1, :] = l
            n1[c, b:b + 1, :] = n
        return 0

    lax.fori_loop(0, conts, own_part, 0)

    sent = list(pending)
    for step in range(2, steps + 1):
        later = ring_step(step)
        lead = len(later) if step == steps else 0
        for got, cp in zip(pending[:lead], later[:lead]):
            got.wait_recv()
            cp.start()
        for got in pending[lead:]:
            got.wait_recv()
        if lead == 0:
            for cp in later:
                cp.start()
        sent += later
        pending = later
    for cp in pending:
        cp.wait_recv()
    for cp in sent:
        cp.wait_send()

    def prefix_part(c, _):
        w = qrow_ref[slot_ref[c] // ANSWERS]
        parts = unpack(kslot[w])
        for i in range(kv):
            kpre[:, i * dim:(i + 1) * dim] = parts[i].astype(BF16)
        vptp[...] = lax.dot_general(
            vpslot[w], expand, TN, preferred_element_type=F32, precision=lax.Precision.HIGHEST
        )
        for b in range(blocks):
            q2 = start_mask(c, b)
            s = lax.dot_general(kpre[...], q2, NT, preferred_element_type=F32)
            m, l, n = softmax_part(s, vptp[...])
            m2[c, b:b + 1, :] = m
            l2[c, b:b + 1, :] = l
            n2[c, b:b + 1, :] = n
        return 0

    lax.fori_loop(0, conts, prefix_part, 0)

    fold = jnp.where(iota((cols, clen), 0) // heads == iota((cols, clen), 1) % tcols, 1.0, 0.0)
    keep = iota((blocks, clen), 1) // tcols == iota((blocks, clen), 0)
    row_id = iota((conts, clen), 0)
    partial = jnp.zeros((conts, clen), F32)
    for c in range(conts):
        ma, mb = m1[c], m2[c]
        m = jnp.maximum(ma, mb)
        ea, eb = jnp.exp2((ma - m) * scale), jnp.exp2((mb - m) * scale)
        ratio = (n1[c] * ea + n2[c] * eb) / (l1[c] * ea + l2[c] * eb)
        y = jnp.dot(ratio, fold, preferred_element_type=F32, precision=lax.Precision.HIGHEST)
        y = jnp.sum(jnp.where(keep, y, 0.0), axis=0, keepdims=True)
        partial = jnp.where(row_id == c, y, partial)
    tslot[me_n] = partial

    choice_rows = wide * quest
    crow = iota((wide, quest, LANES), 0) * quest + iota((wide, quest, LANES), 1)
    clane = iota((wide, quest, LANES), 2)
    term = jnp.zeros((wide, quest, LANES), F32)
    tpos = iota((1, clen), 1)
    for c in range(conts):
        slot = slot_ref[c]
        w = qrow_ref[slot // ANSWERS]
        a = slot % ANSWERS
        val = jnp.sum(jnp.where(tpos < len_ref[c], partial[c:c + 1, :], 0.0), axis=1, keepdims=True)
        term = term + jnp.where((crow == w) & (clane == a), val.reshape(1, 1, 1), 0.0)
    cbuf[...] = term

    def tcopy(i):
        return pltpu.make_async_remote_copy(
            src_ref=tslot.at[me_n], dst_ref=tslot.at[me_n],
            send_sem=tsend.at[i - 1], recv_sem=trecv.at[i - 1],
            device_id={"narrow": lax.rem(me_n + i, narrow)}, device_id_type=MESH,
        )

    def ccopy(i):
        to = peer(i)
        return pltpu.make_async_remote_copy(
            src_ref=cbuf.at[to["wide"]], dst_ref=cslot.at[me],
            send_sem=csend.at[i - 1], recv_sem=crecv.at[i - 1],
            device_id=to, device_id_type=MESH,
        )

    each_peer(total, lambda i: ccopy(i).start())
    each_peer(narrow, lambda i: tcopy(i).start())
    cslot[me] = cbuf[me_w]

    each_peer(narrow, lambda i: tcopy(i).wait())
    tok = tslot[0]
    for i in range(1, narrow):
        tok = tok + tslot[i]
    out_ref[0:conts, :] = tok

    each_peer(total, lambda i: ccopy(i).wait())
    scores = jnp.sum(cslot[...], axis=0)
    live = iota((quest, LANES), 1) < ANSWERS
    masked = jnp.where(live, scores, NEG)
    top = jnp.max(masked, axis=1, keepdims=True)
    norm = jnp.log(jnp.sum(jnp.where(live, jnp.exp(masked - top), 0.0), axis=1, keepdims=True))
    logp = scores - top - norm
    out_ref[conts:conts + quest, :] = logp
    mine = me_w * quest + iota((quest, 1), 0)
    gold = jnp.zeros((quest, 1), jnp.int32)
    for g in range(questions):
        gold = jnp.where(mine == qrow_ref[g], gold_ref[g], gold)
    pick = iota((quest, LANES), 1) == gold
    loss = -jnp.sum(jnp.where(pick, logp, 0.0), axis=1, keepdims=True)
    out_ref[conts + quest:conts + 2 * quest, :] = jnp.broadcast_to(loss, (quest, LANES))


def hand_out(conts, quest, packed_ref, tok_ref, logp_ref, loss_ref):
    tok_ref[...] = packed_ref[0:conts, :]
    logp_ref[...] = packed_ref[conts:conts + quest, :ANSWERS]
    loss_ref[...] = packed_ref[conts + quest:conts + 2 * quest, :1]


def solution(mesh):
    wide, narrow = mesh.shape["wide"], mesh.shape["narrow"]
    total = wide * narrow

    def per_device(q, k, v, prefix, probe, qrow, slot, length, gold):
        conts, clen, heads, dim = q.shape
        kv = k.shape[2]
        quest, _, pref = prefix.shape[:3]
        questions = qrow.shape[0]
        cols = 2 * LANES // heads * heads
        blocks = clen * heads // cols
        sizes = (wide, narrow, conts, clen, heads, kv, dim, quest, pref, questions)
        smem = pl.BlockSpec(memory_space=pltpu.SMEM)
        vmem = pl.BlockSpec(memory_space=pltpu.VMEM)
        anyw = pl.BlockSpec(memory_space=pl.ANY)
        stat = pltpu.VMEM((conts, blocks, cols), F32)
        dma = pltpu.SemaphoreType.DMA
        packed = pl.pallas_call(
            functools.partial(kernel, sizes),
            out_shape=jax.ShapeDtypeStruct((conts + 2 * quest, LANES), F32),
            in_specs=[smem] * 4 + [anyw] * 4 + [vmem],
            out_specs=vmem,
            scratch_shapes=[
                pltpu.VMEM((conts, clen * heads, dim), BF16),
                pltpu.VMEM((conts, clen * kv, dim), BF16),
                pltpu.VMEM((conts, clen * kv, dim), BF16),
                pltpu.VMEM((quest, pref * kv, dim), BF16),
                pltpu.VMEM((wide * quest, pref * kv, dim), BF16),
                pltpu.VMEM((wide * quest, heads, pref), F32),
                pltpu.VMEM((clen * kv, dim), F32),
                pltpu.VMEM((clen, kv * dim), BF16),
                pltpu.VMEM((clen, LANES), F32),
                pltpu.VMEM((pref, kv * dim), BF16),
                pltpu.VMEM((pref, LANES), F32),
                stat, stat, stat, stat, stat, stat,
                pltpu.VMEM((narrow, conts, clen), F32),
                pltpu.VMEM((wide, quest, LANES), F32),
                pltpu.VMEM((total, quest, LANES), F32),
                dma((5,)),
                dma((2 * wide,)), dma((2 * wide,)), dma((2 * wide,)), dma((2 * wide,)),
                dma((narrow - 1,)), dma((narrow - 1,)), dma((total - 1,)), dma((total - 1,)),
            ],
            compiler_params=pltpu.CompilerParams(collective_id=0, has_side_effects=True),
        )(
            qrow, slot, length, gold,
            q.reshape(conts, clen * heads, dim),
            k.reshape(conts, clen * kv, dim),
            v.reshape(conts, clen * kv, dim),
            prefix.reshape(quest, 2, pref * kv, dim),
            probe,
        )
        tok, logp, loss = pl.pallas_call(
            functools.partial(hand_out, conts, quest),
            out_shape=(
                jax.ShapeDtypeStruct((conts, clen), F32),
                jax.ShapeDtypeStruct((quest, ANSWERS), F32),
                jax.ShapeDtypeStruct((quest, 1), F32),
            ),
            in_specs=[vmem],
            out_specs=(vmem, vmem, vmem),
        )(packed)
        return tok, logp, loss.reshape(quest)

    return jax.shard_map(
        per_device,
        mesh=mesh,
        in_specs=(
            P(("groups", "wide"), None, "narrow", None),
            P(("groups", "wide"), None, "narrow", None),
            P(("groups", "wide"), None, "narrow", None),
            P(("groups", "wide"), None, None, "narrow", None),
            P("narrow", None),
            P("groups"),
            P(("groups", "wide")),
            P(("groups", "wide")),
            P("groups"),
        ),
        out_specs=(P(("groups", "wide"), None), P(("groups", "wide"), None), P(("groups", "wide"))),
        check_vma=False,
    )
```
